32 devices in a mesh: gx: 4 (over y, core), gy: 4 (over z), gz: 2 (over x).
Axes of the slice: x: 2, y: 2, z: 4, core: 2. Of those that a mesh axis runs over, the one named last changes fastest.
Arguments:
- positions: float32 [3, 4, 8, 16, 128], P(None, 'gx', 'gy', 'gz'), may hold values from 0 to 1
- velocities: float32 [3, 4, 8, 16, 128], P(None, 'gx', 'gy', 'gz'), may hold values from -6 to 6
- occupancy: int32 [4, 8, 16], P('gx', 'gy', 'gz'), may hold values from 0 to 128, as said below
- mover_pos: float32 [3, 12, 4, 2, 128], P(None, 'gx', 'gy', 'gz'), may hold values from 0 to 1
- mover_vel: float32 [3, 12, 4, 2, 128], P(None, 'gx', 'gy', 'gz'), may hold values from -6 to 6
- mover_count: int32 [12, 4, 2], P('gx', 'gy', 'gz'), may hold values from 1 to 128
- mover_owner: int32 [12, 4, 2], P('gx', 'gy', 'gz'), may hold values from 0 to 3, as said below
- mover_cell: int32 [12, 4, 2], P('gx', 'gy', 'gz'), may hold values from 0 to 15, as said below
Outputs:
- new_positions: float32 [3, 4, 8, 16, 128], P(None, 'gx', 'gy', 'gz')
- new_velocities: float32 [3, 4, 8, 16, 128], P(None, 'gx', 'gy', 'gz')
The draws below stay inside these ranges and needn't reach their ends.
Inputs may be any that keep to these rules, and one draw needn't show every extreme that they name: `mover_owner`: all leaving blocks of one device go to one owner in the device's own line along gx; at most 6 blocks arrive at one device, and in every draw some device takes 2 * 3 and some takes none. `mover_cell`: the cells named by the blocks that arrive at one device are distinct, and their occupancy is 0. Exactly 6 cells of each device have occupancy 0; every other cell holds 32 or more particles, and one cell of each device holds 128.
All inputs are finite; a program needn't handle non-finite values.
Results may differ from the reference program's by a relative error of at most 0.0001.
Values sent between devices are 32-bit elements; how exact they have to be, the bound alone decides.
A program may use at most 64 MiB of HBM per device.

```python
import math
import jax
import jax.numpy as jnp
from jax import lax

CX = 1
CY = 2
CZ = 8
SLOTS = 128
CAP = 3
NX = 4
NY = 8
NZ = 16
MOVERS = 12
N_GX = 4
N_GY = 4
N_GZ = 2


def column_plan(key):
    cell_total = CX * CY * CZ

    def one_column(column_key):
        keys = jax.random.split(column_key, 5)
        sigma = jax.random.permutation(keys[0], N_GX)
        heavy = jax.random.randint(keys[1], (N_GX // 2,), 0, 2).at[0].set(1)
        loads = jnp.zeros((N_GX,), jnp.int32).at[sigma[0::2]].set(1 + heavy).at[sigma[1::2]].set(1 - heavy)
        ceiling = jnp.cumsum(loads)
        starts = ceiling - loads
        position = jnp.arange(N_GX, dtype=jnp.int32)
        receiver = jnp.sum((ceiling[None, :] <= position[:, None]).astype(jnp.int32), axis=1)
        ordering = jax.random.permutation(keys[2], N_GX)
        owners = receiver[ordering]
        ranks = ordering - starts[owners]
        shuffles = jax.vmap(lambda sub_key: jax.random.permutation(sub_key, cell_total))(jax.random.split(keys[3], N_GX))
        picks = ranks[:, None] * CAP + jnp.arange(CAP, dtype=jnp.int32)[None, :]
        cells_to = shuffles[owners[:, None], picks]
        fills = jax.random.randint(keys[4], (N_GX, cell_total), SLOTS // 4, SLOTS + 1)
        rows_all = jnp.arange(N_GX, dtype=jnp.int32)[:, None]
        fills = fills.at[rows_all, shuffles[:, 2 * CAP:2 * CAP + 1]].set(SLOTS)
        fills = fills.at[rows_all, shuffles[:, :2 * CAP]].set(0)
        owner_table = jnp.broadcast_to(owners[:, None], (N_GX, CAP))
        return (owner_table, cells_to, fills)
    column_keys = jax.random.split(jax.random.fold_in(key, 11), N_GY * N_GZ)
    owners, cells_to, fills = jax.vmap(one_column)(column_keys)
    owners = owners.reshape(N_GY, N_GZ, N_GX, CAP)
    cells_to = cells_to.reshape(N_GY, N_GZ, N_GX, CAP)
    fills = fills.reshape(N_GY, N_GZ, N_GX, CX, CY, CZ)
    return (owners, cells_to, fills)


def draw_mover_owner(key, part):
    owners, cells_to, fills = column_plan(key)
    return owners.transpose(2, 3, 0, 1).reshape(N_GX * CAP, N_GY, N_GZ).astype(jnp.int32)


def draw_mover_cell(key, part):
    owners, cells_to, fills = column_plan(key)
    return cells_to.transpose(2, 3, 0, 1).reshape(N_GX * CAP, N_GY, N_GZ).astype(jnp.int32)


def draw_occupancy(key, part):
    owners, cells_to, fills = column_plan(key)
    return fills.transpose(2, 3, 0, 4, 1, 5).reshape(CX * N_GX, CY * N_GY, CZ * N_GZ).astype(jnp.int32)


def touch_ends(result, own_key, low, high):
    longest = result.shape.index(max(result.shape))
    spots = []
    for shift in (0, 1):
        where = [jax.random.randint(jax.random.fold_in(own_key, axis), (), 0, length) for axis, length in enumerate(result.shape)]
        where[longest] = (where[longest] + shift) % result.shape[longest]
        spots.append(tuple(where))
    return result.at[spots[0]].set(low).at[spots[1]].set(high)


def level_of(rng, dims, pieces, low, top_value):
    gain, own = 1.0, jax.random.fold_in(rng, 6)
    for dim, shards_of in pieces:
        draws = jnp.exp(jax.random.uniform(jax.random.fold_in(own, dim), (shards_of,), jnp.float32, low / len(pieces), top_value / len(pieces)))
        gain = gain * jnp.repeat(draws, dims[dim] // shards_of).reshape([-1 if axis == dim else 1 for axis in range(len(dims))])
    return gain


def gaussian(key, dims, width, limit, cuts=(), held_as=jnp.bfloat16):
    values = width * jax.random.normal(key, dims, jnp.float32)
    if cuts:
        values = values * level_of(key, dims, cuts, -0.22, 0.18)
    return jnp.clip(values, -limit, limit).astype(held_as)


def setup_inputs(seed: int = 0) -> dict:
    splits = jax.random.split(jax.random.key(seed), 9)
    return {
        "positions": jnp.clip(1.0 * jax.random.uniform(splits[0], (3, NX, NY, NZ, SLOTS), jnp.float32) ** level_of(splits[0], (3, NX, NY, NZ, SLOTS), ((1, 4), (2, 4), (3, 2)), -0.2, 0.2), 0.0, 1.0),
        "velocities": gaussian(splits[1], (3, NX, NY, NZ, SLOTS), 1.0, 6.0, ((1, 4), (2, 4), (3, 2)), jnp.float32),
        "occupancy": draw_occupancy(jax.random.fold_in(splits[8], 71), 0),
        "mover_pos": jnp.clip(1.0 * jax.random.uniform(splits[3], (3, MOVERS, N_GY, N_GZ, SLOTS), jnp.float32) ** level_of(splits[3], (3, MOVERS, N_GY, N_GZ, SLOTS), ((1, 4), (2, 4), (3, 2)), -0.2, 0.2), 0.0, 1.0),
        "mover_vel": gaussian(splits[4], (3, MOVERS, N_GY, N_GZ, SLOTS), 1.0, 6.0, ((1, 4), (2, 4), (3, 2)), jnp.float32),
        "mover_count": touch_ends(jax.random.randint(splits[5], (MOVERS, N_GY, N_GZ), 1, SLOTS + 1), jax.random.fold_in(splits[5], 1), 1, SLOTS).astype(jnp.int32),
        "mover_owner": draw_mover_owner(jax.random.fold_in(splits[8], 71), 0),
        "mover_cell": draw_mover_cell(jax.random.fold_in(splits[8], 71), 0),
    }


eps_soft = 0.05
kick_step = 0.02
drift_step = 0.1
far_away = 1000.0

def pair_force(targets, sources, displace):
    separation = sources[:, :, None, :] + displace[:, None, None, None] - targets[:, :, :, None]
    squared = lax.optimization_barrier(jnp.sum(separation * separation, axis=0))
    inside = jnp.maximum(1.0 - squared, 0.0)
    weight = inside * inside / ((squared + eps_soft) * jnp.sqrt(squared + eps_soft))
    return lax.optimization_barrier(jnp.sum(weight[None] * separation, axis=3))

def reference(positions, velocities, occupancy, mover_pos, mover_vel, mover_count, mover_owner, mover_cell):
    plane = CY * CZ
    row_x = (mover_owner * CX + mover_cell // plane).astype(jnp.int32)
    row_y = (jnp.arange(N_GY, dtype=jnp.int32)[None, :, None] * CY + mover_cell // CZ % CY).astype(jnp.int32)
    row_z = (jnp.arange(N_GZ, dtype=jnp.int32)[None, None, :] * CZ + mover_cell % CZ).astype(jnp.int32)
    positions = positions.at[:, row_x, row_y, row_z, :].set(mover_pos)
    velocities = velocities.at[:, row_x, row_y, row_z, :].set(mover_vel)
    occupancy = occupancy.at[row_x, row_y, row_z].set(mover_count)
    live = jnp.arange(SLOTS, dtype=jnp.int32)[None, None, None, :] < occupancy[..., None]
    sources = jnp.where(live[None], positions, far_away)
    padded = jnp.pad(sources, ((0, 0), (1, 1), (1, 1), (1, 1), (0, 0)), mode='wrap')
    cell_total = NX * NY * NZ
    block_size = math.gcd(cell_total, 256)
    block_total = cell_total // block_size
    targets = positions.reshape(3, block_total, block_size, SLOTS).transpose(1, 0, 2, 3)
    force = jnp.zeros((block_total, 3, block_size, SLOTS), jnp.float32)
    for offset_id in range(27):
        step_x = offset_id // 9
        step_y = offset_id // 3 % 3
        step_z = offset_id % 3
        window = padded[:, step_x:step_x + NX, step_y:step_y + NY, step_z:step_z + NZ, :]
        window = window.reshape(3, block_total, block_size, SLOTS).transpose(1, 0, 2, 3)
        displace = jnp.array([step_x - 1, step_y - 1, step_z - 1], jnp.float32)
        force = force + lax.map(lambda paired: pair_force(paired[0], paired[1], displace), (targets, window))
    force = force.transpose(1, 0, 2, 3).reshape(3, NX, NY, NZ, SLOTS)
    new_velocities = jnp.where(live[None], velocities + kick_step * force, 0.0)
    new_positions = jnp.where(live[None], positions + drift_step * new_velocities, 0.0)
    return (new_positions, new_velocities)
```

```python
import functools

import jax
import jax.numpy as jnp
from jax import lax
from jax.experimental import pallas as pl
from jax.experimental.pallas import tpu as pltpu
from jax.sharding import PartitionSpec as P

eps_soft = 0.05
kick_step = 0.02
drift_step = 0.1
far_away = 1000.0


def with_halo(block, sides, width):
    for axis, dim in sides:
        count = lax.axis_size(axis)
        forward = [(i, (i + 1) % count) for i in range(count)]
        backward = [(target, source) for source, target in forward]
        low = lax.ppermute(
            lax.slice_in_dim(block, block.shape[dim] - width, None, axis=dim), axis, forward
        )
        high = lax.ppermute(lax.slice_in_dim(block, 0, width, axis=dim), axis, backward)
        block = jnp.concatenate([low, block, high], axis=dim)
    return block


def force_kernel(
    size_x, size_y, size_z, lead, occ_s, src_ref, pos_ref, vel_ref, occ_v, npos_ref, nvel_ref, wide, acc
):
    cells = size_x * size_y * size_z
    slots = pos_ref.shape[2]
    groups = slots // 8
    hy, hz = size_y + 2, size_z + 2

    index = lax.broadcasted_iota(jnp.int32, (cells, 1), 0)
    corner = (
        index // (size_y * size_z) + 1,
        index // size_z % size_y + 1,
        index % size_z + 1,
    )
    for k in range(3):
        moved = pos_ref[k] + corner[k].astype(jnp.float32)
        padded = jnp.concatenate([moved, jnp.zeros((slots - cells, slots), jnp.float32)], 0)
        flipped = padded.T
        for t in range(cells):
            wide[k, t] = jnp.broadcast_to(flipped[:, t : t + 1], (slots, slots))

    def cell_step(t, carry):
        cx = t // (size_y * size_z)
        cy = t // size_z % size_y
        cz = t % size_z
        first = (cx * hy + cy) * hz + cz
        count = occ_s[t]

        def group_step(g, carry):
            rows = pl.ds(pl.multiple_of(g * lead, lead), lead)
            px, py, pz = wide[0, t, rows, :], wide[1, t, rows, :], wide[2, t, rows, :]
            fx = fy = fz = jnp.zeros((lead, slots), jnp.float32)
            for ex in range(3):
                for ey in range(3):
                    for ez in range(3):
                        cell = first + (ex * hy + ey) * hz + ez
                        rx = src_ref[0, pl.ds(cell, 1), :] - px
                        ry = src_ref[1, pl.ds(cell, 1), :] - py
                        rz = src_ref[2, pl.ds(cell, 1), :] - pz
                        t2 = (rx * rx + ry * ry) + (rz * rz + eps_soft)
                        u = jnp.maximum((1.0 + eps_soft) - t2, 0.0)
                        y = lax.rsqrt(t2)
                        a = u * y
                        w = a * a * y
                        fx = fx + w * rx
                        fy = fy + w * ry
                        fz = fz + w * rz
            acc[0, t, rows, :] = fx
            acc[1, t, rows, :] = fy
            acc[2, t, rows, :] = fz
            return carry

        lax.fori_loop(0, (count + lead - 1) // lead, group_step, 0)
        return carry

    lax.fori_loop(0, cells, cell_step, 0)

    live = lax.broadcasted_iota(jnp.int32, (cells, slots), 1) < occ_v[...]
    for k in range(3):
        force = jnp.concatenate(
            [jnp.sum(acc[k, t].T, axis=0, keepdims=True) for t in range(cells)], 0
        )
        vel = jnp.where(live, vel_ref[k] + kick_step * force, 0.0)
        nvel_ref[k] = vel
        npos_ref[k] = jnp.where(live, pos_ref[k] + drift_step * vel, 0.0)


def forces(padded, targets, speeds, occupied, shape):
    size_x, size_y, size_z = shape
    cells, slots = targets.shape[1:]
    lead = 16
    out = jax.ShapeDtypeStruct(targets.shape, jnp.float32)
    vmem = pl.BlockSpec(memory_space=pltpu.VMEM)
    return pl.pallas_call(
        functools.partial(force_kernel, size_x, size_y, size_z, lead),
        out_shape=(out, out),
        in_specs=[pl.BlockSpec(memory_space=pltpu.SMEM), vmem, vmem, vmem, vmem],
        out_specs=(vmem, vmem),
        scratch_shapes=[
            pltpu.VMEM((3, cells, slots, slots), jnp.float32),
            pltpu.VMEM((3, cells, slots, slots), jnp.float32),
        ],
        compiler_params=pltpu.CompilerParams(vmem_limit_bytes=32 * 1024 * 1024),
        name="forces",
    )(occupied, padded, targets, speeds, occupied[:, None])


def per_device(
    positions, velocities, occupancy, mover_pos, mover_vel, mover_count, mover_owner, mover_cell
):
    size_x, size_y, size_z = (positions.shape[1], positions.shape[2], positions.shape[3])
    slot_total = positions.shape[4]
    cell_total = size_x * size_y * size_z
    leaving = mover_pos.shape[1]
    holdings = jnp.concatenate([positions, velocities], 0).reshape(6, cell_total, slot_total)
    blocks = jnp.concatenate([mover_pos, mover_vel], 0).reshape(6, leaving, slot_total)
    owners = mover_owner.reshape(leaving)
    cells_to = mover_cell.reshape(leaving)
    counts = mover_count.reshape(leaving)
    labels = jnp.stack([owners, cells_to, counts]).astype(jnp.float32)
    arrived, arrived_labels = (
        lax.all_gather(blocks, "gx", axis=1, tiled=True),
        lax.all_gather(labels, "gx", axis=1, tiled=True),
    )
    is_mine = arrived_labels[0].astype(jnp.int32) == lax.axis_index("gx")
    landing = jnp.where(is_mine, arrived_labels[1].astype(jnp.int32), cell_total)
    filled = arrived_labels[2].astype(jnp.int32)
    holdings = holdings.at[:, landing].set(arrived, mode="drop")
    occupied = occupancy.reshape(cell_total).at[landing].set(filled, mode="drop")
    live = lax.broadcasted_iota(jnp.int32, (cell_total, slot_total), 1) < occupied[:, None]
    sources = jnp.where(live[None], holdings[:3], far_away).reshape(
        3, size_x, size_y, size_z, slot_total
    )
    padded = with_halo(sources, (("gx", 1), ("gy", 2), ("gz", 3)), 1)
    frame = jnp.stack(
        [lax.broadcasted_iota(jnp.float32, padded.shape[1:4], k) for k in range(3)]
    )
    padded = (padded + frame[..., None]).reshape(3, -1, slot_total)
    shape_out = (3, size_x, size_y, size_z, slot_total)
    new_positions, new_velocities = forces(
        padded, holdings[:3], holdings[3:], occupied, (size_x, size_y, size_z)
    )
    return (new_positions.reshape(shape_out), new_velocities.reshape(shape_out))


def solution(mesh):
    cells = P(None, "gx", "gy", "gz", None)
    labels = P("gx", "gy", "gz")
    return jax.shard_map(
        per_device,
        mesh=mesh,
        in_specs=(cells, cells, labels, cells, cells, labels, labels, labels),
        out_specs=(cells, cells),
        check_vma=False,
    )
```

```python
import functools

import jax
import jax.numpy as jnp
from jax import lax
from jax.experimental import pallas as pl
from jax.experimental.pallas import tpu as pltpu
from jax.sharding import PartitionSpec as P

eps_soft = 0.05
kick_step = 0.02
drift_step = 0.1
far_away = 1000.0


def offsets(count):
    return sorted({0, 1 % count, count - 1})


def exchange_kernel(axes, shape, leaving, pos_ref, mov_ref, halo_ref, all_ref, sems, *rest):
    send, recv, msend, mrecv, local = sems, *rest
    nx, ny, nz = axes
    dims = shape
    ys, zs = offsets(ny), offsets(nz)
    me = [lax.axis_index(name) for name in ("gx", "gy", "gz")]

    def device(step):
        return tuple(lax.rem(m + s, n) for m, s, n in zip(me, step, axes))

    def peers(body):
        for oy in ys:
            for oz in zs:
                start = 1 if oy == 0 and oz == 0 else 0

                def one(ox, carry, oy=oy, oz=oz):
                    body(ox, oy, oz)
                    return carry

                if nx <= 4:
                    for ox in range(start, nx):
                        one(ox, 0)
                else:
                    lax.fori_loop(start, nx, one, 0)

    def halo_copy(step):
        source, target = [slice(None)], [slice(None)]
        for d, size in zip(step, dims):
            if d == 0:
                source.append(pl.ds(0, size))
                target.append(pl.ds(1, size))
            elif d == 1:
                source.append(pl.ds(size - 1, 1))
                target.append(pl.ds(0, 1))
            else:
                source.append(pl.ds(0, 1))
                target.append(pl.ds(size + 1, 1))
        number = (step[0] + 1) * 9 + (step[1] + 1) * 3 + step[2] + 1
        return pltpu.make_async_remote_copy(
            src_ref=pos_ref.at[tuple(source)],
            dst_ref=halo_ref.at[tuple(target)],
            send_sem=send.at[number],
            recv_sem=recv.at[number],
            device_id=device([d % n for d, n in zip(step, axes)]),
            device_id_type=pl.DeviceIdType.MESH,
        )

    def mover_copy(ox, oy, oz):
        cy, cz = ys.index((-oy) % ny), zs.index((-oz) % nz)
        row = ((cy * len(zs) + cz) * nx + me[0]) * leaving
        planes = 7 if oy == 0 and oz == 0 else 4
        number = (cy * len(zs) + cz) * nx + ox
        return pltpu.make_async_remote_copy(
            src_ref=mov_ref.at[pl.ds(0, planes)],
            dst_ref=all_ref.at[pl.ds(0, planes), pl.ds(row, leaving)],
            send_sem=msend.at[number],
            recv_sem=mrecv.at[number],
            device_id=device((ox, oy, oz)),
            device_id_type=pl.DeviceIdType.MESH,
        )

    barrier = pltpu.get_barrier_semaphore()
    peers(
        lambda ox, oy, oz: pl.semaphore_signal(
            barrier,
            inc=1,
            device_id=device((ox, oy, oz)),
            device_id_type=pl.DeviceIdType.MESH,
        )
    )
    own = pltpu.make_async_copy(
        pos_ref,
        halo_ref.at[:, pl.ds(1, dims[0]), pl.ds(1, dims[1]), pl.ds(1, dims[2])],
        local.at[0],
    )
    own_movers = pltpu.make_async_copy(
        mov_ref, all_ref.at[:, pl.ds(me[0] * leaving, leaving)], local.at[1]
    )
    own.start()
    own_movers.start()
    pl.semaphore_wait(barrier, nx * len(ys) * len(zs) - 1)
    steps = [
        (dx, dy, dz)
        for dx in (-1, 0, 1)
        for dy in (-1, 0, 1)
        for dz in (-1, 0, 1)
        if (dx, dy, dz) != (0, 0, 0)
    ]
    steps.sort(key=lambda step: -sum(abs(d) for d in step))
    peers(lambda ox, oy, oz: mover_copy(ox, oy, oz).start())
    for step in steps:
        halo_copy(step).start()
    own.wait()
    own_movers.wait()
    peers(lambda ox, oy, oz: mover_copy(ox, oy, oz).wait())
    for step in steps:
        halo_copy(step).wait()


def exchange(pos, mov):
    axes = tuple(lax.axis_size(name) for name in ("gx", "gy", "gz"))
    shape, leaving, slots = pos.shape[1:4], mov.shape[1], mov.shape[3]
    lines = len(offsets(axes[1])) * len(offsets(axes[2]))
    padded = (3,) + tuple(size + 2 for size in shape) + (1, slots)
    gathered = (7, lines * axes[0] * leaving, 1, slots)
    vmem = pl.BlockSpec(memory_space=pltpu.VMEM)
    return pl.pallas_call(
        functools.partial(exchange_kernel, axes, shape, leaving),
        out_shape=(
            pltpu.VMEM(padded, jnp.float32),
            pltpu.VMEM(gathered, jnp.float32),
        ),
        in_specs=[vmem, vmem],
        out_specs=(pl.BlockSpec(memory_space=pl.ANY), pl.BlockSpec(memory_space=pl.ANY)),
        scratch_shapes=[
            pltpu.SemaphoreType.DMA((27,)),
            pltpu.SemaphoreType.DMA((27,)),
            pltpu.SemaphoreType.DMA((lines * axes[0],)),
            pltpu.SemaphoreType.DMA((lines * axes[0],)),
            pltpu.SemaphoreType.DMA((2,)),
        ],
        compiler_params=pltpu.CompilerParams(collective_id=0, has_side_effects=True),
        name="exchange",
    )(pos, mov)


def force_kernel(
    size_x, size_y, size_z, lead, occ_s, raw_ref, mov_ref, land_ref, vel_ref, occ_v,
    npos_ref, nvel_ref, wide, acc, src_ref, pos_ref
):
    cells = size_x * size_y * size_z
    slots = pos_ref.shape[2]
    hy, hz = size_y + 2, size_z + 2

    halo_cells = raw_ref.shape[1]
    halo = lax.broadcasted_iota(jnp.int32, (halo_cells, land_ref.shape[1]), 0)
    landed = (halo == land_ref[...]).astype(jnp.float32)
    any_landed = jnp.sum(landed, axis=1, keepdims=True) > 0.5
    halo_index = lax.broadcasted_iota(jnp.int32, (halo_cells, 1), 0)
    frame = (halo_index // (hy * hz), halo_index // hz % hy, halo_index % hz)
    for k in range(3):
        arrived = jnp.dot(
            landed,
            mov_ref[k],
            precision=lax.Precision.HIGHEST,
            preferred_element_type=jnp.float32,
        )
        here = jnp.where(any_landed, arrived, raw_ref[k])
        starts = [
            ((x + 1) * hy + y + 1) * hz + 1 for x in range(size_x) for y in range(size_y)
        ]
        pos_ref[k] = jnp.concatenate([here[at : at + size_z] for at in starts], 0)
        src_ref[k] = here + frame[k].astype(jnp.float32)

    index = lax.broadcasted_iota(jnp.int32, (cells, 1), 0)
    corner = (
        index // (size_y * size_z) + 1,
        index // size_z % size_y + 1,
        index % size_z + 1,
    )
    for k in range(3):
        moved = pos_ref[k] + corner[k].astype(jnp.float32)
        padded = jnp.concatenate([moved, jnp.zeros((slots - cells, slots), jnp.float32)], 0)
        flipped = padded.T
        for t in range(cells):
            wide[k, t] = jnp.broadcast_to(flipped[:, t : t + 1], (slots, slots))

    def cell_step(t, carry):
        cx = t // (size_y * size_z)
        cy = t // size_z % size_y
        cz = t % size_z
        first = (cx * hy + cy) * hz + cz
        count = occ_s[t]

        def group_step(g, carry):
            rows = pl.ds(pl.multiple_of(g * lead, lead), lead)
            px, py, pz = wide[0, t, rows, :], wide[1, t, rows, :], wide[2, t, rows, :]
            fx = fy = fz = jnp.zeros((lead, slots), jnp.float32)
            for ex in range(3):
                for ey in range(3):
                    for ez in range(3):
                        cell = first + (ex * hy + ey) * hz + ez
                        rx = src_ref[0, pl.ds(cell, 1), :] - px
                        ry = src_ref[1, pl.ds(cell, 1), :] - py
                        rz = src_ref[2, pl.ds(cell, 1), :] - pz
                        t2 = (rx * rx + ry * ry) + (rz * rz + eps_soft)
                        u = jnp.maximum((1.0 + eps_soft) - t2, 0.0)
                        y = lax.rsqrt(t2)
                        a = u * y
                        w = a * a * y
                        fx = fx + w * rx
                        fy = fy + w * ry
                        fz = fz + w * rz
            acc[0, t, rows, :] = fx
            acc[1, t, rows, :] = fy
            acc[2, t, rows, :] = fz
            return carry

        lax.fori_loop(0, (count + lead - 1) // lead, group_step, 0)
        return carry

    lax.fori_loop(0, cells, cell_step, 0)

    live = lax.broadcasted_iota(jnp.int32, (cells, slots), 1) < occ_v[...]
    for k in range(3):
        force = jnp.concatenate(
            [jnp.sum(acc[k, t].T, axis=0, keepdims=True) for t in range(cells)], 0
        )
        vel = jnp.where(live, vel_ref[k] + kick_step * force, 0.0)
        nvel_ref[k] = vel
        npos_ref[k] = jnp.where(live, pos_ref[k] + drift_step * vel, 0.0)


def forces(padded, movers, land, speeds, occupied, shape):
    size_x, size_y, size_z = shape
    cells, slots = speeds.shape[1:]
    lead = 16
    out = jax.ShapeDtypeStruct(speeds.shape, jnp.float32)
    vmem = pl.BlockSpec(memory_space=pltpu.VMEM)
    return pl.pallas_call(
        functools.partial(force_kernel, size_x, size_y, size_z, lead),
        out_shape=(out, out),
        in_specs=[pl.BlockSpec(memory_space=pltpu.SMEM)] + [vmem] * 5,
        out_specs=(vmem, vmem),
        scratch_shapes=[
            pltpu.VMEM((3, cells, slots, slots), jnp.float32),
            pltpu.VMEM((3, cells, slots, slots), jnp.float32),
            pltpu.VMEM(padded.shape, jnp.float32),
            pltpu.VMEM(speeds.shape, jnp.float32),
        ],
        compiler_params=pltpu.CompilerParams(vmem_limit_bytes=32 * 1024 * 1024),
        name="forces",
    )(occupied, padded, movers, land, speeds, occupied[:, None])


def per_device(
    positions, velocities, occupancy, mover_pos, mover_vel, mover_count, mover_owner, mover_cell
):
    shape = positions.shape[1:4]
    size_x, size_y, size_z = shape
    slots = positions.shape[4]
    cells = size_x * size_y * size_z
    leaving = mover_pos.shape[1]
    nx, ny, nz = (lax.axis_size(name) for name in ("gx", "gy", "gz"))
    slot = lax.broadcasted_iota(jnp.int32, (1, 1, 1, slots), 3)
    pos = jnp.where((slot < occupancy[..., None])[None], positions, far_away)
    counts = mover_count.reshape(leaving)
    mpos = jnp.where(
        slot[0, 0] < counts[:, None], mover_pos.reshape(3, leaving, slots), far_away
    )
    lane = slot[0, 0]
    label = jnp.where(
        lane == 0,
        mover_owner.reshape(leaving, 1),
        jnp.where(lane == 1, mover_cell.reshape(leaving, 1), counts[:, None]),
    ).astype(jnp.float32)
    mov = jnp.concatenate([mpos, label[None], mover_vel.reshape(3, leaving, slots)], 0)
    padded, movers = exchange(
        pos.reshape(3, *shape, 1, slots), mov.reshape(7, leaving, 1, slots)
    )
    padded = padded.reshape(3, -1, slots)
    movers = movers.reshape(7, -1, slots)

    ys, zs = offsets(ny), offsets(nz)
    labels = movers[3, :, :3].astype(jnp.int32).reshape(len(ys), len(zs), nx * leaving, 3)
    owner, cell, filled = labels[..., 0], labels[..., 1], labels[..., 2]

    def place(local, offset, size, count):
        here = jnp.where(offset == 0, local + 1, -1)
        if count > 1:
            here = jnp.where((offset == 1) & (local == 0), size + 1, here)
            here = jnp.where((offset == count - 1) & (local == size - 1), 0, here)
        return here

    off_y = jnp.array(ys, jnp.int32)[:, None, None]
    off_z = jnp.array(zs, jnp.int32)[None, :, None]
    off_x = lax.rem(owner - lax.axis_index("gx") + nx, nx)
    at_x = place(cell // (size_y * size_z), off_x, size_x, nx)
    at_y = place(cell // size_z % size_y, off_y, size_y, ny)
    at_z = place(cell % size_z, off_z, size_z, nz)
    inside = (at_x >= 0) & (at_y >= 0) & (at_z >= 0)
    land = jnp.where(inside, (at_x * (size_y + 2) + at_y) * (size_z + 2) + at_z, -1)
    land = land.reshape(1, -1)

    mine = (owner[0, 0] == lax.axis_index("gx"))[:, None] & (
        cell[0, 0][:, None] == jnp.arange(cells, dtype=jnp.int32)[None, :]
    )
    occupied = occupancy.reshape(cells) + jnp.sum(
        jnp.where(mine, filled[0, 0][:, None], 0), axis=0
    )
    own = velocities.reshape(3, cells, slots)
    arrived = jnp.sum(
        jnp.where(mine[None, :, :, None], movers[4:, : nx * leaving, None, :], 0.0), axis=1
    )
    speeds = jnp.where(jnp.any(mine, axis=0)[None, :, None], arrived, own)
    new_positions, new_velocities = forces(padded, movers, land, speeds, occupied, shape)
    shape_out = (3, *shape, slots)
    return (new_positions.reshape(shape_out), new_velocities.reshape(shape_out))


def solution(mesh):
    cells = P(None, "gx", "gy", "gz", None)
    labels = P("gx", "gy", "gz")
    return jax.shard_map(
        per_device,
        mesh=mesh,
        in_specs=(cells, cells, labels, cells, cells, labels, labels, labels),
        out_specs=(cells, cells),
        check_vma=False,
    )
```

```python
import functools

import jax
import jax.numpy as jnp
from jax import lax
from jax.experimental import pallas as pl
from jax.experimental.pallas import tpu as pltpu
from jax.sharding import PartitionSpec as P

eps_soft = 0.05
kick_step = 0.02
drift_step = 0.1
far_away = 1000.0


def offsets(count):
    return sorted({0, 1 % count, count - 1})


def exchange_kernel(
    axes, shape, leaving, occ_s, count_s, owner_s, cell_s, raw_ref, mpos_ref, mvel_ref,
    halo_ref, all_ref, pos_ref, mov_ref, send, recv, msend, mrecv, local
):
    nx, ny, nz = axes
    dims = shape
    ys, zs = offsets(ny), offsets(nz)
    me = [lax.axis_index(name) for name in ("gx", "gy", "gz")]

    def device(step):
        return tuple(lax.rem(m + s, n) for m, s, n in zip(me, step, axes))

    def peers(body):
        for oy in ys:
            for oz in zs:
                start = 1 if oy == 0 and oz == 0 else 0

                def one(ox, carry, oy=oy, oz=oz):
                    body(ox, oy, oz)
                    return carry

                if nx <= 4:
                    for ox in range(start, nx):
                        one(ox, 0)
                else:
                    lax.fori_loop(start, nx, one, 0)

    def halo_copy(step):
        source, target = [slice(None)], [slice(None)]
        for d, size in zip(step, dims):
            if d == 0:
                source.append(pl.ds(0, size))
                target.append(pl.ds(1, size))
            elif d == 1:
                source.append(pl.ds(size - 1, 1))
                target.append(pl.ds(0, 1))
            else:
                source.append(pl.ds(0, 1))
                target.append(pl.ds(size + 1, 1))
        number = (step[0] + 1) * 9 + (step[1] + 1) * 3 + step[2] + 1
        return pltpu.make_async_remote_copy(
            src_ref=pos_ref.at[tuple(source)],
            dst_ref=halo_ref.at[tuple(target)],
            send_sem=send.at[number],
            recv_sem=recv.at[number],
            device_id=device([d % n for d, n in zip(step, axes)]),
            device_id_type=pl.DeviceIdType.MESH,
        )

    def mover_copy(ox, oy, oz):
        cy, cz = ys.index((-oy) % ny), zs.index((-oz) % nz)
        row = ((cy * len(zs) + cz) * nx + me[0]) * leaving
        planes = 7 if oy == 0 and oz == 0 else 4
        number = (cy * len(zs) + cz) * nx + ox
        return pltpu.make_async_remote_copy(
            src_ref=mov_ref.at[pl.ds(0, planes)],
            dst_ref=all_ref.at[pl.ds(0, planes), pl.ds(row, leaving)],
            send_sem=msend.at[number],
            recv_sem=mrecv.at[number],
            device_id=device((ox, oy, oz)),
            device_id_type=pl.DeviceIdType.MESH,
        )

    barrier = pltpu.get_barrier_semaphore()
    peers(
        lambda ox, oy, oz: pl.semaphore_signal(
            barrier,
            inc=1,
            device_id=device((ox, oy, oz)),
            device_id_type=pl.DeviceIdType.MESH,
        )
    )
    lane = lax.broadcasted_iota(jnp.int32, (1, pos_ref.shape[-1]), 1)
    for x in range(dims[0]):
        for y in range(dims[1]):
            for z in range(dims[2]):
                live = lane < occ_s[x, y, z]
                for k in range(3):
                    pos_ref[k, x, y, z] = jnp.where(live, raw_ref[k, x, y, z], far_away)
    for b in range(leaving):
        live = lane < count_s[b]
        for k in range(3):
            mov_ref[k, b] = jnp.where(live, mpos_ref[k, b], far_away)
            mov_ref[4 + k, b] = mvel_ref[k, b]
        label = jnp.where(lane == 0, owner_s[b], cell_s[b])
        mov_ref[3, b] = label.astype(jnp.float32)
    own = pltpu.make_async_copy(
        pos_ref,
        halo_ref.at[:, pl.ds(1, dims[0]), pl.ds(1, dims[1]), pl.ds(1, dims[2])],
        local.at[0],
    )
    own_movers = pltpu.make_async_copy(
        mov_ref, all_ref.at[:, pl.ds(me[0] * leaving, leaving)], local.at[1]
    )
    own.start()
    own_movers.start()
    pl.semaphore_wait(barrier, nx * len(ys) * len(zs) - 1)
    steps = [
        (dx, dy, dz)
        for dx in (-1, 0, 1)
        for dy in (-1, 0, 1)
        for dz in (-1, 0, 1)
        if (dx, dy, dz) != (0, 0, 0)
    ]
    steps.sort(key=lambda step: -sum(abs(d) for d in step))
    peers(lambda ox, oy, oz: mover_copy(ox, oy, oz).start())
    for step in steps:
        halo_copy(step).start()
    own.wait()
    own_movers.wait()
    peers(lambda ox, oy, oz: mover_copy(ox, oy, oz).wait())
    for step in steps:
        halo_copy(step).wait()


def exchange(occupancy, count, owner, cell, pos, mpos, mvel):
    axes = tuple(lax.axis_size(name) for name in ("gx", "gy", "gz"))
    shape, leaving, slots = pos.shape[1:4], mpos.shape[1], mpos.shape[3]
    lines = len(offsets(axes[1])) * len(offsets(axes[2]))
    padded = (3,) + tuple(size + 2 for size in shape) + (1, slots)
    gathered = (7, lines * axes[0] * leaving, 1, slots)
    vmem = pl.BlockSpec(memory_space=pltpu.VMEM)
    return pl.pallas_call(
        functools.partial(exchange_kernel, axes, shape, leaving),
        out_shape=(
            pltpu.VMEM(padded, jnp.float32),
            pltpu.VMEM(gathered, jnp.float32),
        ),
        in_specs=[pl.BlockSpec(memory_space=pltpu.SMEM)] * 4 + [vmem] * 3,
        out_specs=(pl.BlockSpec(memory_space=pl.ANY), pl.BlockSpec(memory_space=pl.ANY)),
        scratch_shapes=[
            pltpu.VMEM(pos.shape, jnp.float32),
            pltpu.VMEM((7, leaving, 1, slots), jnp.float32),
            pltpu.SemaphoreType.DMA((27,)),
            pltpu.SemaphoreType.DMA((27,)),
            pltpu.SemaphoreType.DMA((lines * axes[0],)),
            pltpu.SemaphoreType.DMA((lines * axes[0],)),
            pltpu.SemaphoreType.DMA((2,)),
        ],
        compiler_params=pltpu.CompilerParams(collective_id=0, has_side_effects=True),
        name="exchange",
    )(occupancy, count, owner, cell, pos, mpos, mvel)


def place(local, offset, size, count):
    here = jnp.where(offset == 0, local + 1, -1)
    if count > 1:
        here = jnp.where((offset == 1) & (local == 0), size + 1, here)
        here = jnp.where((offset == count - 1) & (local == size - 1), 0, here)
    return here


def pick(number, values):
    out = jnp.full_like(number, values[0])
    for i, value in enumerate(values[1:]):
        out = jnp.where(number == i + 1, value, out)
    return out


def force_kernel(
    axes, shape, leaving, lead, raw_ref, mov_ref, vel_ref, npos_ref, nvel_ref,
    wide, acc, src_ref, pos_ref, cnt_s
):
    size_x, size_y, size_z = shape
    nx, ny, nz = axes
    cells = size_x * size_y * size_z
    slots = pos_ref.shape[2]
    hy, hz = size_y + 2, size_z + 2
    halo_cells = (size_x + 2) * hy * hz
    blocks = mov_ref.shape[1]
    ys, zs = offsets(ny), offsets(nz)

    labels = mov_ref[3, :, 0, :].astype(jnp.int32)
    owner, cell = labels[:, 0:1], labels[:, 1:2]
    column = lax.broadcasted_iota(jnp.int32, (blocks, 1), 0) // (nx * leaving)
    off_x = owner - lax.axis_index("gx")
    off_x = jnp.where(off_x < 0, off_x + nx, off_x)
    at_x = place(cell // (size_y * size_z), off_x, size_x, nx)
    at_y = place(cell // size_z % size_y, pick(column // len(zs), ys), size_y, ny)
    at_z = place(cell % size_z, pick(column % len(zs), zs), size_z, nz)
    inside = (at_x >= 0) & (at_y >= 0) & (at_z >= 0)
    land = jnp.where(inside, (at_x * hy + at_y) * hz + at_z, -1)
    halo_pad = -(-halo_cells // 128) * 128
    block_pad = -(-blocks // 128) * 128

    def padded_rows(value):
        extra = block_pad - blocks
        if extra == 0:
            return value
        return jnp.concatenate([value, jnp.zeros((extra, value.shape[1]), value.dtype)], 0)

    spread = lax.broadcasted_iota(jnp.int32, (blocks, halo_pad), 1) == land
    landed = padded_rows(spread.astype(jnp.float32)).T[:halo_cells]
    any_landed = jnp.sum(landed, axis=1, keepdims=True) > 0.5
    halo_index = lax.broadcasted_iota(jnp.int32, (halo_cells, 1), 0)
    frame = (halo_index // (hy * hz), halo_index // hz % hy, halo_index % hz)
    starts = [((x + 1) * hy + y + 1) * hz + 1 for x in range(size_x) for y in range(size_y)]

    def inner(value):
        return jnp.concatenate([value[at : at + size_z] for at in starts], 0)

    def arrive(hot, rows):
        return jnp.dot(
            hot, rows, precision=lax.Precision.HIGHEST, preferred_element_type=jnp.float32
        )

    for k in range(3):
        arrived = arrive(landed, padded_rows(mov_ref[k, :, 0, :]))
        here = jnp.where(any_landed, arrived, raw_ref[k, :, 0, :])
        pos_ref[k] = inner(here)
        src_ref[k] = here + frame[k].astype(jnp.float32)
    for t in range(cells):
        alive = (pos_ref[0, t : t + 1, :] < 0.5 * far_away).astype(jnp.int32)
        cnt_s[t] = jnp.sum(alive)

    index = lax.broadcasted_iota(jnp.int32, (cells, 1), 0)
    corner = (
        index // (size_y * size_z) + 1,
        index // size_z % size_y + 1,
        index % size_z + 1,
    )
    for k in range(3):
        moved = pos_ref[k] + corner[k].astype(jnp.float32)
        padded = jnp.concatenate([moved, jnp.zeros((slots - cells, slots), jnp.float32)], 0)
        flipped = padded.T
        for t in range(cells):
            wide[k, t] = jnp.broadcast_to(flipped[:, t : t + 1], (slots, slots))

    def cell_step(t, carry):
        cx = t // (size_y * size_z)
        cy = t // size_z % size_y
        cz = t % size_z
        first = (cx * hy + cy) * hz + cz
        count = cnt_s[t]

        def group_step(g, carry):
            rows = pl.ds(pl.multiple_of(g * lead, lead), lead)
            px, py, pz = wide[0, t, rows, :], wide[1, t, rows, :], wide[2, t, rows, :]
            fx = fy = fz = jnp.zeros((lead, slots), jnp.float32)
            for ex in range(3):
                for ey in range(3):
                    for ez in range(3):
                        cell = first + (ex * hy + ey) * hz + ez
                        rx = src_ref[0, pl.ds(cell, 1), :] - px
                        ry = src_ref[1, pl.ds(cell, 1), :] - py
                        rz = src_ref[2, pl.ds(cell, 1), :] - pz
                        t2 = (rx * rx + ry * ry) + (rz * rz + eps_soft)
                        u = jnp.maximum((1.0 + eps_soft) - t2, 0.0)
                        y = lax.rsqrt(t2)
                        a = u * y
                        w = a * a * y
                        fx = fx + w * rx
                        fy = fy + w * ry
                        fz = fz + w * rz
            acc[0, t, rows, :] = fx
            acc[1, t, rows, :] = fy
            acc[2, t, rows, :] = fz
            return carry

        lax.fori_loop(0, (count + lead - 1) // lead, group_step, 0)
        return carry

    lax.fori_loop(0, cells, cell_step, 0)

    live = pos_ref[0] < 0.5 * far_away
    hot, came = inner(landed), inner(any_landed.astype(jnp.float32)) > 0.5
    line = lax.broadcasted_iota(jnp.int32, (blocks, 1), 0) < nx * leaving
    for k in range(3):
        force = jnp.concatenate(
            [jnp.sum(acc[k, t].T, axis=0, keepdims=True) for t in range(cells)], 0
        )
        moved = arrive(hot, padded_rows(jnp.where(line, mov_ref[4 + k, :, 0, :], 0.0)))
        vel = jnp.where(came, moved, vel_ref[k])
        vel = jnp.where(live, vel + kick_step * force, 0.0)
        nvel_ref[k] = vel
        npos_ref[k] = jnp.where(live, pos_ref[k] + drift_step * vel, 0.0)


def forces(padded, movers, speeds, shape, leaving):
    axes = tuple(lax.axis_size(name) for name in ("gx", "gy", "gz"))
    cells, slots = speeds.shape[1:]
    lead = 16
    out = jax.ShapeDtypeStruct(speeds.shape, jnp.float32)
    vmem = pl.BlockSpec(memory_space=pltpu.VMEM)
    return pl.pallas_call(
        functools.partial(force_kernel, axes, shape, leaving, lead),
        out_shape=(out, out),
        in_specs=[vmem] * 3,
        out_specs=(vmem, vmem),
        scratch_shapes=[
            pltpu.VMEM((3, cells, slots, slots), jnp.float32),
            pltpu.VMEM((3, cells, slots, slots), jnp.float32),
            pltpu.VMEM((3, padded.shape[1], slots), jnp.float32),
            pltpu.VMEM(speeds.shape, jnp.float32),
            pltpu.SMEM((cells,), jnp.int32),
        ],
        compiler_params=pltpu.CompilerParams(vmem_limit_bytes=32 * 1024 * 1024),
        name="forces",
    )(padded, movers, speeds)


def per_device(
    positions, velocities, occupancy, mover_pos, mover_vel, mover_count, mover_owner, mover_cell
):
    shape = positions.shape[1:4]
    slots = positions.shape[4]
    leaving = mover_pos.shape[1]
    padded, movers = exchange(
        occupancy,
        mover_count.reshape(leaving),
        mover_owner.reshape(leaving),
        mover_cell.reshape(leaving),
        positions.reshape(3, *shape, 1, slots),
        mover_pos.reshape(3, leaving, 1, slots),
        mover_vel.reshape(3, leaving, 1, slots),
    )
    new_positions, new_velocities = forces(
        padded.reshape(3, -1, 1, slots), movers, velocities.reshape(3, -1, slots), shape, leaving
    )
    shape_out = (3, *shape, slots)
    return (new_positions.reshape(shape_out), new_velocities.reshape(shape_out))


def solution(mesh):
    cells = P(None, "gx", "gy", "gz", None)
    labels = P("gx", "gy", "gz")
    return jax.shard_map(
        per_device,
        mesh=mesh,
        in_specs=(cells, cells, labels, cells, cells, labels, labels, labels),
        out_specs=(cells, cells),
        check_vma=False,
    )
```

```python
import functools

import jax
import jax.numpy as jnp
from jax import lax
from jax.experimental import pallas as pl
from jax.experimental.pallas import tpu as pltpu
from jax.sharding import PartitionSpec as P

eps_soft = 0.05
kick_step = 0.02
drift_step = 0.1
far_away = 1000.0


def offsets(count):
    return sorted({0, 1 % count, count - 1})


def exchange_kernel(
    axes, shape, leaving, occ_s, count_s, owner_s, cell_s, raw_ref, mpos_ref, mvel_ref,
    halo_ref, all_ref, pos_ref, mov_ref, send, recv, msend, mrecv, local
):
    nx, ny, nz = axes
    dims = shape
    ys, zs = offsets(ny), offsets(nz)
    me = [lax.axis_index(name) for name in ("gx", "gy", "gz")]

    known = {}

    def wrapped(axis, step):
        if isinstance(step, int):
            if (axis, step) in known:
                return known[axis, step]
            if step == 0:
                return me[axis]
        moved = me[axis] + step
        moved = jnp.where(moved >= axes[axis], moved - axes[axis], moved)
        if isinstance(step, int):
            known[axis, step] = moved
        return moved

    for axis in (1, 2):
        for step in offsets(axes[axis]):
            wrapped(axis, step)
    for step in range(axes[0]) if axes[0] <= 4 else offsets(axes[0]):
        wrapped(0, step)

    def device(step):
        return tuple(wrapped(axis, s) for axis, s in enumerate(step))

    def peers(body):
        for oy in ys:
            for oz in zs:
                start = 1 if oy == 0 and oz == 0 else 0

                def one(ox, carry, oy=oy, oz=oz):
                    body(ox, oy, oz)
                    return carry

                if nx <= 4:
                    for ox in range(start, nx):
                        one(ox, 0)
                else:
                    lax.fori_loop(start, nx, one, 0)

    def halo_copy(step):
        source, target = [slice(None)], [slice(None)]
        for d, size in zip(step, dims):
            if d == 0:
                source.append(pl.ds(0, size))
                target.append(pl.ds(1, size))
            elif d == 1:
                source.append(pl.ds(size - 1, 1))
                target.append(pl.ds(0, 1))
            else:
                source.append(pl.ds(0, 1))
                target.append(pl.ds(size + 1, 1))
        number = (step[0] + 1) * 9 + (step[1] + 1) * 3 + step[2] + 1
        return pltpu.make_async_remote_copy(
            src_ref=pos_ref.at[tuple(source)],
            dst_ref=halo_ref.at[tuple(target)],
            send_sem=send.at[number],
            recv_sem=recv.at[number],
            device_id=device([d % n for d, n in zip(step, axes)]),
            device_id_type=pl.DeviceIdType.MESH,
        )

    def mover_copy(ox, oy, oz):
        cy, cz = ys.index((-oy) % ny), zs.index((-oz) % nz)
        row = ((cy * len(zs) + cz) * nx + me[0]) * leaving
        planes = 7 if oy == 0 and oz == 0 else 4
        number = (cy * len(zs) + cz) * nx + ox
        return pltpu.make_async_remote_copy(
            src_ref=mov_ref.at[pl.ds(0, planes)],
            dst_ref=all_ref.at[pl.ds(0, planes), pl.ds(row, leaving)],
            send_sem=msend.at[number],
            recv_sem=mrecv.at[number],
            device_id=device((ox, oy, oz)),
            device_id_type=pl.DeviceIdType.MESH,
        )

    barrier = pltpu.get_barrier_semaphore()
    peers(
        lambda ox, oy, oz: pl.semaphore_signal(
            barrier,
            inc=1,
            device_id=device((ox, oy, oz)),
            device_id_type=pl.DeviceIdType.MESH,
        )
    )
    lane = lax.broadcasted_iota(jnp.int32, (1, pos_ref.shape[-1]), 1)
    for x in range(dims[0]):
        for y in range(dims[1]):
            for z in range(dims[2]):
                live = lane < occ_s[x, y, z]
                for k in range(3):
                    pos_ref[k, x, y, z] = jnp.where(live, raw_ref[k, x, y, z], far_away)
    for b in range(leaving):
        live = lane < count_s[b]
        for k in range(3):
            mov_ref[k, b] = jnp.where(live, mpos_ref[k, b], far_away)
            mov_ref[4 + k, b] = mvel_ref[k, b]
        label = jnp.where(lane == 0, owner_s[b], cell_s[b])
        mov_ref[3, b] = label.astype(jnp.float32)
    own = pltpu.make_async_copy(
        pos_ref,
        halo_ref.at[:, pl.ds(1, dims[0]), pl.ds(1, dims[1]), pl.ds(1, dims[2])],
        local.at[0],
    )
    own_movers = pltpu.make_async_copy(
        mov_ref, all_ref.at[:, pl.ds(me[0] * leaving, leaving)], local.at[1]
    )
    own.start()
    own_movers.start()
    pl.semaphore_wait(barrier, nx * len(ys) * len(zs) - 1)
    steps = [
        (dx, dy, dz)
        for dx in (-1, 0, 1)
        for dy in (-1, 0, 1)
        for dz in (-1, 0, 1)
        if (dx, dy, dz) != (0, 0, 0)
    ]
    steps.sort(key=lambda step: -sum(abs(d) for d in step))
    halos = [halo_copy(step) for step in steps]
    for copy in halos:
        copy.start()
    peers(lambda ox, oy, oz: mover_copy(ox, oy, oz).start())
    own.wait()
    own_movers.wait()
    for copy in halos:
        copy.wait()
    peers(lambda ox, oy, oz: mover_copy(ox, oy, oz).wait())


def exchange(occupancy, count, owner, cell, pos, mpos, mvel):
    axes = tuple(lax.axis_size(name) for name in ("gx", "gy", "gz"))
    shape, leaving, slots = pos.shape[1:4], mpos.shape[1], mpos.shape[3]
    lines = len(offsets(axes[1])) * len(offsets(axes[2]))
    padded = (3,) + tuple(size + 2 for size in shape) + (1, slots)
    gathered = (7, lines * axes[0] * leaving, 1, slots)
    vmem = pl.BlockSpec(memory_space=pltpu.VMEM)
    return pl.pallas_call(
        functools.partial(exchange_kernel, axes, shape, leaving),
        out_shape=(
            pltpu.VMEM(padded, jnp.float32),
            pltpu.VMEM(gathered, jnp.float32),
        ),
        in_specs=[pl.BlockSpec(memory_space=pltpu.SMEM)] * 4 + [vmem] * 3,
        out_specs=(pl.BlockSpec(memory_space=pl.ANY), pl.BlockSpec(memory_space=pl.ANY)),
        scratch_shapes=[
            pltpu.VMEM(pos.shape, jnp.float32),
            pltpu.VMEM((7, leaving, 1, slots), jnp.float32),
            pltpu.SemaphoreType.DMA((27,)),
            pltpu.SemaphoreType.DMA((27,)),
            pltpu.SemaphoreType.DMA((lines * axes[0],)),
            pltpu.SemaphoreType.DMA((lines * axes[0],)),
            pltpu.SemaphoreType.DMA((2,)),
        ],
        compiler_params=pltpu.CompilerParams(collective_id=0, has_side_effects=True),
        name="exchange",
    )(occupancy, count, owner, cell, pos, mpos, mvel)


def place(local, offset, size, count):
    here = jnp.where(offset == 0, local + 1, -1)
    if count > 1:
        here = jnp.where((offset == 1) & (local == 0), size + 1, here)
        here = jnp.where((offset == count - 1) & (local == size - 1), 0, here)
    return here


def pick(number, values):
    out = jnp.full_like(number, values[0])
    for i, value in enumerate(values[1:]):
        out = jnp.where(number == i + 1, value, out)
    return out


def force_kernel(
    axes, shape, leaving, lead, raw_ref, mov_ref, vel_ref, npos_ref, nvel_ref,
    wide, acc, src_ref, pos_ref, cnt_s
):
    size_x, size_y, size_z = shape
    nx, ny, nz = axes
    cells = size_x * size_y * size_z
    slots = pos_ref.shape[2]
    hy, hz = size_y + 2, size_z + 2
    halo_cells = (size_x + 2) * hy * hz
    blocks = mov_ref.shape[1]
    ys, zs = offsets(ny), offsets(nz)

    labels = mov_ref[3, :, 0, :].astype(jnp.int32)
    owner, cell = labels[:, 0:1], labels[:, 1:2]
    column = lax.broadcasted_iota(jnp.int32, (blocks, 1), 0) // (nx * leaving)
    off_x = owner - lax.axis_index("gx")
    off_x = jnp.where(off_x < 0, off_x + nx, off_x)
    at_x = place(cell // (size_y * size_z), off_x, size_x, nx)
    at_y = place(cell // size_z % size_y, pick(column // len(zs), ys), size_y, ny)
    at_z = place(cell % size_z, pick(column % len(zs), zs), size_z, nz)
    inside = (at_x >= 0) & (at_y >= 0) & (at_z >= 0)
    land = jnp.where(inside, (at_x * hy + at_y) * hz + at_z, -1)
    halo_pad = -(-halo_cells // 128) * 128
    block_pad = -(-blocks // 128) * 128

    def padded_rows(value):
        extra = block_pad - blocks
        if extra == 0:
            return value
        return jnp.concatenate([value, jnp.zeros((extra, value.shape[1]), value.dtype)], 0)

    spread = lax.broadcasted_iota(jnp.int32, (blocks, halo_pad), 1) == land
    landed = padded_rows(spread.astype(jnp.float32)).T[:halo_cells]
    any_landed = jnp.sum(landed, axis=1, keepdims=True) > 0.5
    halo_index = lax.broadcasted_iota(jnp.int32, (halo_cells, 1), 0)
    frame = (halo_index // (hy * hz), halo_index // hz % hy, halo_index % hz)
    starts = [((x + 1) * hy + y + 1) * hz + 1 for x in range(size_x) for y in range(size_y)]

    def inner(value):
        return jnp.concatenate([value[at : at + size_z] for at in starts], 0)

    def arrive(hot, rows):
        return jnp.dot(
            hot, rows, precision=lax.Precision.HIGHEST, preferred_element_type=jnp.float32
        )

    for k in range(3):
        arrived = arrive(landed, padded_rows(mov_ref[k, :, 0, :]))
        here = jnp.where(any_landed, arrived, raw_ref[k, :, 0, :])
        pos_ref[k] = inner(here)
        src_ref[k] = here + frame[k].astype(jnp.float32)
    for t in range(cells):
        alive = (pos_ref[0, t : t + 1, :] < 0.5 * far_away).astype(jnp.int32)
        cnt_s[t] = jnp.sum(alive)

    index = lax.broadcasted_iota(jnp.int32, (cells, 1), 0)
    corner = (
        index // (size_y * size_z) + 1,
        index // size_z % size_y + 1,
        index % size_z + 1,
    )
    for k in range(3):
        moved = pos_ref[k] + corner[k].astype(jnp.float32)
        padded = jnp.concatenate([moved, jnp.zeros((slots - cells, slots), jnp.float32)], 0)
        flipped = padded.T
        for t in range(cells):
            wide[k, t] = jnp.broadcast_to(flipped[:, t : t + 1], (slots, slots))

    def cell_step(t, carry):
        cx = t // (size_y * size_z)
        cy = t // size_z % size_y
        cz = t % size_z
        first = (cx * hy + cy) * hz + cz
        count = cnt_s[t]

        def group_step(g, carry):
            rows = pl.ds(pl.multiple_of(g * lead, lead), lead)
            px, py, pz = wide[0, t, rows, :], wide[1, t, rows, :], wide[2, t, rows, :]
            fx = fy = fz = jnp.zeros((lead, slots), jnp.float32)
            for ex in range(3):
                for ey in range(3):
                    for ez in range(3):
                        cell = first + (ex * hy + ey) * hz + ez
                        rx = src_ref[0, pl.ds(cell, 1), :] - px
                        ry = src_ref[1, pl.ds(cell, 1), :] - py
                        rz = src_ref[2, pl.ds(cell, 1), :] - pz
                        t2 = (rx * rx + ry * ry) + (rz * rz + eps_soft)
                        u = jnp.maximum((1.0 + eps_soft) - t2, 0.0)
                        y = lax.rsqrt(t2)
                        a = u * y
                        w = a * a * y
                        fx = fx + w * rx
                        fy = fy + w * ry
                        fz = fz + w * rz
            acc[0, t, rows, :] = fx
            acc[1, t, rows, :] = fy
            acc[2, t, rows, :] = fz
            return carry

        lax.fori_loop(0, (count + lead - 1) // lead, group_step, 0)
        return carry

    lax.fori_loop(0, cells, cell_step, 0)

    live = pos_ref[0] < 0.5 * far_away
    hot, came = inner(landed), inner(any_landed.astype(jnp.float32)) > 0.5
    line = lax.broadcasted_iota(jnp.int32, (blocks, 1), 0) < nx * leaving
    for k in range(3):
        force = jnp.concatenate(
            [jnp.sum(acc[k, t].T, axis=0, keepdims=True) for t in range(cells)], 0
        )
        moved = arrive(hot, padded_rows(jnp.where(line, mov_ref[4 + k, :, 0, :], 0.0)))
        vel = jnp.where(came, moved, vel_ref[k])
        vel = jnp.where(live, vel + kick_step * force, 0.0)
        nvel_ref[k] = vel
        npos_ref[k] = jnp.where(live, pos_ref[k] + drift_step * vel, 0.0)


def forces(padded, movers, speeds, shape, leaving):
    axes = tuple(lax.axis_size(name) for name in ("gx", "gy", "gz"))
    cells, slots = speeds.shape[1:]
    lead = 16
    out = jax.ShapeDtypeStruct(speeds.shape, jnp.float32)
    vmem = pl.BlockSpec(memory_space=pltpu.VMEM)
    return pl.pallas_call(
        functools.partial(force_kernel, axes, shape, leaving, lead),
        out_shape=(out, out),
        in_specs=[vmem] * 3,
        out_specs=(vmem, vmem),
        scratch_shapes=[
            pltpu.VMEM((3, cells, slots, slots), jnp.float32),
            pltpu.VMEM((3, cells, slots, slots), jnp.float32),
            pltpu.VMEM((3, padded.shape[1], slots), jnp.float32),
            pltpu.VMEM(speeds.shape, jnp.float32),
            pltpu.SMEM((cells,), jnp.int32),
        ],
        compiler_params=pltpu.CompilerParams(vmem_limit_bytes=32 * 1024 * 1024),
        name="forces",
    )(padded, movers, speeds)


def per_device(
    positions, velocities, occupancy, mover_pos, mover_vel, mover_count, mover_owner, mover_cell
):
    shape = positions.shape[1:4]
    slots = positions.shape[4]
    leaving = mover_pos.shape[1]
    padded, movers = exchange(
        occupancy,
        mover_count.reshape(leaving),
        mover_owner.reshape(leaving),
        mover_cell.reshape(leaving),
        positions.reshape(3, *shape, 1, slots),
        mover_pos.reshape(3, leaving, 1, slots),
        mover_vel.reshape(3, leaving, 1, slots),
    )
    new_positions, new_velocities = forces(
        padded.reshape(3, -1, 1, slots), movers, velocities.reshape(3, -1, slots), shape, leaving
    )
    shape_out = (3, *shape, slots)
    return (new_positions.reshape(shape_out), new_velocities.reshape(shape_out))


def solution(mesh):
    cells = P(None, "gx", "gy", "gz", None)
    labels = P("gx", "gy", "gz")
    return jax.shard_map(
        per_device,
        mesh=mesh,
        in_specs=(cells, cells, labels, cells, cells, labels, labels, labels),
        out_specs=(cells, cells),
        check_vma=False,
    )
```
